32 devices in a mesh: seq: 8 (over z, core), tp: 4 (over y, x).
Axes of the slice: x: 2, y: 2, z: 4, core: 2. Of those that a mesh axis runs over, the one named last changes fastest.
Arguments:
- hidden: bfloat16 [4096, 2048], P(('seq', 'tp')), may hold values from -5 to 5
- w_qkv: bfloat16 [2048, 3, 2048], P(None, None, 'tp'), may hold values from -0.125 to 0.125
- w_gate: bfloat16 [2048, 2048], P(None, 'tp'), may hold values from -0.125 to 0.125
- w_decay_beta: bfloat16 [2048, 2, 16], P(None, None, 'tp'), may hold values from -0.7 to 0.7
- conv_weight: bfloat16 [4, 3, 2048], P(None, None, 'tp'), may hold values from -2 to 2
- decay_rate: float32 [16], P('tp'), may hold values from 2e-05 to 0.05
- dt_bias: float32 [16], P('tp'), may hold values from -1 to 1
- norm_gain: float32 [128], replicated, may hold values from 0.1 to 1.9
Outputs:
- core: bfloat16 [4096, 2048], P('seq', 'tp')
The draws below stay inside these ranges and needn't reach their ends.
All inputs are finite; a program needn't handle non-finite values.
Results may differ from the reference program's by a relative error of at most 0.01.
Values may be sent and summed in bfloat16 or wider, within the bound.
A program may use at most 64 MiB of HBM per device.

```python
import math
import jax
import jax.numpy as jnp
from jax import lax

D = 2048
H = 16
DH = 128
KERNEL = 4
SEQ = 4096


def direction_signs(key):
    return jax.random.rademacher(jax.random.fold_in(key, 71), (D,), dtype=jnp.float32)


def slow_heads(key):
    order = jax.random.permutation(jax.random.fold_in(key, 72), H)
    count = 3 * H // 8
    return (order < count).astype(jnp.float32)


def draw_hidden(key, part):
    signs = direction_signs(key)
    noise_key = jax.random.fold_in(key, 73)
    noise = 0.9 * jax.random.truncated_normal(noise_key, -5.0, 5.0, (SEQ, D), jnp.float32)
    offset = 0.4
    return (noise + offset * signs[None, :]).astype(jnp.bfloat16)


def draw_w_decay_beta(key, part):
    signs = direction_signs(key)
    slow = slow_heads(key)
    base = jax.random.truncated_normal(jax.random.fold_in(key, 74), -5.0, 5.0, (D, 2, H), jnp.float32)
    base = base * (1.0 / math.sqrt(D))
    strength = jax.random.uniform(jax.random.fold_in(key, 75), (H,), jnp.float32, 10.0, 13.0)
    slow_column = -strength[None, :] * signs[:, None] * (1.0 / D) + 0.3 * base[:, 1, :]
    beta_column = slow[None, :] * slow_column + (1.0 - slow[None, :]) * base[:, 1, :]
    return jnp.stack([base[:, 0, :], beta_column], axis=1).astype(jnp.bfloat16)


def draw_decay_rate(key, part):
    slow = slow_heads(key)
    fraction = jax.random.uniform(jax.random.fold_in(key, 76), (H,), jnp.float32, 0.0, 1.0)
    slow_rate = jnp.exp(math.log(2e-05) + fraction * (math.log(0.00015) - math.log(2e-05)))
    fast_rate = jnp.exp(math.log(0.002) + fraction * (math.log(0.05) - math.log(0.002)))
    return jnp.where(slow > 0.5, slow_rate, fast_rate).astype(jnp.float32)


def levels(own_key, dims, shards, low, high):
    level = 1.0
    for axis_at, shards_of in shards:
        draws = jax.random.uniform(jax.random.fold_in(jax.random.fold_in(own_key, 6), axis_at), (shards_of,), jnp.float32, low / len(shards), high / len(shards))
        level = level * jnp.repeat(jnp.exp(draws), dims[axis_at] // shards_of).reshape((-1,) + (1,) * (len(dims) - 1 - axis_at))
    return level


def scatter_about(stream_key, extent, deviation, limit, shards=(), held_as=jnp.bfloat16):
    loudness = levels(stream_key, extent, shards, -0.22, 0.18) if shards else 1.0
    entries = jax.random.normal(stream_key, extent, jnp.float32) * deviation * loudness
    return jnp.minimum(jnp.maximum(entries, -limit), limit).astype(held_as)


def setup_inputs(seed: int = 0) -> dict:
    arg_keys = jax.random.split(jax.random.key(seed), 9)
    return {
        "hidden": draw_hidden(jax.random.fold_in(arg_keys[8], 71), 0),
        "w_qkv": scatter_about(arg_keys[1], (D, 3, H * DH), D ** -0.5, 0.125, ((2, 4),)),
        "w_gate": scatter_about(arg_keys[2], (D, H * DH), D ** -0.5, 0.125, ((1, 4),)),
        "w_decay_beta": draw_w_decay_beta(jax.random.fold_in(arg_keys[8], 71), 0),
        "conv_weight": scatter_about(arg_keys[4], (KERNEL, 3, H * DH), 0.5, 2.0, ((2, 4),)),
        "decay_rate": draw_decay_rate(jax.random.fold_in(arg_keys[8], 71), 0),
        "dt_bias": jnp.clip(jax.random.uniform(arg_keys[6], (H,), jnp.float32, -1.0, 1.0) * levels(arg_keys[6], (H,), ((0, 4),), -0.4, 0.0), -1.0, 1.0),
        "norm_gain": jnp.clip(1.0 + 0.18 * jax.random.normal(arg_keys[7], (DH,), jnp.float32), 0.1, 1.9),
    }


def unit_rows(matrix):
    return matrix * lax.rsqrt(lax.optimization_barrier(jnp.sum(matrix * matrix, axis=-1, keepdims=True)) + 1e-06)

def reference(hidden, w_qkv, w_gate, w_decay_beta, conv_weight, decay_rate, dt_bias, norm_gain):
    seq_total = hidden.shape[0]
    columns = H * DH
    projected = jnp.dot(hidden, w_qkv.reshape(D, 3 * columns), preferred_element_type=jnp.float32)
    projected = projected.astype(jnp.bfloat16).reshape(seq_total, 3, columns)
    padded = jnp.concatenate([jnp.zeros((KERNEL - 1, 3, columns), jnp.bfloat16), projected], axis=0)
    convolved = jnp.zeros((seq_total, 3, columns), jnp.float32)
    for offset in range(KERNEL):
        convolved = convolved + padded[offset:offset + seq_total].astype(jnp.float32) * conv_weight[offset].astype(jnp.float32)
    activated = jax.nn.silu(convolved).astype(jnp.bfloat16)
    scalars = jnp.dot(hidden, w_decay_beta.reshape(D, 2 * H), preferred_element_type=jnp.float32).reshape(seq_total, 2, H)
    log_decay = -decay_rate * jax.nn.softplus(scalars[:, 0] + dt_bias)
    write_rate = jax.nn.sigmoid(scalars[:, 1])
    branches = activated.astype(jnp.float32).reshape(seq_total, 3, H, DH)
    inv_root = 1.0 / math.sqrt(DH)
    queries = unit_rows(branches[:, 0]) * inv_root
    keys_in = unit_rows(branches[:, 1])
    values_in = branches[:, 2]

    def advance(state_history, inputs):
        single_query, single_key, value_row, decay_row, rate_row = inputs
        state_history = jnp.exp(decay_row)[:, None, None] * state_history
        retrieved_value = jnp.einsum('cd,cdn->cn', single_key, state_history, precision=lax.Precision.HIGHEST)
        state_history = state_history + rate_row[:, None, None] * single_key[:, :, None] * (value_row - retrieved_value)[:, None, :]
        return (state_history, jnp.einsum('cd,cdn->cn', single_query, state_history, precision=lax.Precision.HIGHEST))
    start_state = jnp.zeros((H, DH, DH), jnp.float32)
    _, state_output = lax.scan(advance, start_state, (queries, keys_in, values_in, log_decay, write_rate))
    gate_linear = jnp.dot(hidden, w_gate, preferred_element_type=jnp.float32).reshape(seq_total, H, DH)
    rms_scale = lax.rsqrt(lax.optimization_barrier(jnp.mean(state_output * state_output, axis=-1, keepdims=True)) + 1e-06)
    core = state_output * rms_scale * norm_gain * jax.nn.silu(gate_linear)
    return core.reshape(seq_total, columns).astype(jnp.bfloat16)
```

```python
import functools
import math

import jax
import jax.numpy as jnp
from jax import lax
from jax.experimental import pallas as pl
from jax.experimental.pallas import tpu as pltpu
from jax.sharding import PartitionSpec as P

MESH = pl.DeviceIdType.MESH
CHUNK = 128
RIM = 16
NT = (((1,), (1,)), ((), ()))
TN = (((0,), (0,)), ((), ()))


def low(value):
    return value.astype(jnp.bfloat16)


def dot(left, right, dims=(((1,), (0,)), ((), ()))):
    return lax.dot_general(low(left), low(right), dims, preferred_element_type=jnp.float32)


def peer_of(me, step, count):
    if count & (count - 1):
        return lax.rem(me + step, count)
    bit = 1
    while bit < count:
        if step & bit:
            me = me + bit - 2 * bit * lax.rem(me // bit, 2)
        bit *= 2
    return me


def silu(value):
    return value / (1.0 + jnp.exp(-value))


def unit_rows(matrix):
    return matrix * lax.rsqrt(jnp.sum(matrix * matrix, axis=-1, keepdims=True) + 1e-06)


def kernel(
    n_seq, n_tp, rate_ref, bias_ref, hidden, w_qkv, w_gate, wdb_ref, conv_ref, gain_ref, out_ref,
    tokens, rim, weights, proj, state, outs, deltas, st_in, st_out,
    tok_send, tok_recv, w_sem, rim_send, rim_recv, st_send, st_recv,
):
    seq, me = lax.axis_index("seq"), lax.axis_index("tp")
    rows = hidden.shape[0]
    total = tokens.shape[0]
    heads = rate_ref.shape[0]
    head_dim = gain_ref.shape[1]
    taps = conv_ref.shape[1]
    last_tp, last_seq = n_tp - 1, n_seq - 1

    own = pltpu.make_async_copy(hidden, tokens.at[pl.ds(me * rows, rows)], tok_recv.at[0])
    own.start()
    loads = [pltpu.make_async_copy(w_qkv.at[b], weights.at[b], w_sem.at[b]) for b in range(3)]
    loads.append(pltpu.make_async_copy(w_gate, weights.at[3], w_sem.at[3]))
    for load in loads:
        load.start()

    barrier = pltpu.get_barrier_semaphore()

    def greet(where):
        pl.semaphore_signal(barrier, inc=1, device_id=where, device_id_type=MESH)

    for step in range(1, n_tp):
        greet({"tp": peer_of(me, step, n_tp)})

    @pl.when(seq > 0)
    def _():
        greet({"seq": seq - 1})

        @pl.when(me < last_tp)
        def _():
            greet({"seq": seq - 1, "tp": last_tp})

    @pl.when(seq < last_seq)
    def _():
        greet({"seq": seq + 1})

    before = (seq + last_seq) // n_seq
    after = (2 * last_seq - seq) // n_seq
    tail_owner = (me + 1) // n_tp
    pl.semaphore_wait(barrier, last_tp + before + after + after * tail_owner * last_tp)

    def token_copy(step):
        peer = peer_of(me, step, n_tp)
        return pltpu.make_async_remote_copy(
            src_ref=hidden,
            dst_ref=tokens.at[pl.ds(me * rows, rows)],
            send_sem=tok_send.at[step],
            recv_sem=tok_recv.at[step],
            device_id={"tp": peer},
            device_id_type=MESH,
        )

    def rim_copy(target):
        return pltpu.make_async_remote_copy(
            src_ref=hidden.at[pl.ds(rows - RIM, RIM)],
            dst_ref=rim,
            send_sem=rim_send.at[target],
            recv_sem=rim_recv,
            device_id={"seq": seq + 1, "tp": target},
            device_id_type=MESH,
        )

    for step in range(1, n_tp):
        token_copy(step).start()

    @pl.when(jnp.logical_and(seq < last_seq, me == last_tp))
    def _():
        for target in range(n_tp):
            rim_copy(target).start()

    @pl.when(seq == 0)
    def _():
        rim[...] = jnp.zeros_like(rim)
        st_in[...] = jnp.zeros_like(st_in)

    for load in loads:
        load.wait()

    def project(block, at):
        def one(b, carry):
            full = jnp.dot(block, weights[b], preferred_element_type=jnp.float32)
            rounded = full.astype(jnp.bfloat16).astype(jnp.float32)
            proj[b, pl.ds(pl.multiple_of(at, 16), block.shape[0]), :] = jnp.where(b < 3, rounded, full)
            return carry

        lax.fori_loop(0, 4, one, 0)

    for step in range(n_tp):
        if step == 0:
            own.wait()
        else:
            token_copy(step).wait_recv()
        if n_tp & (n_tp - 1):
            slot = lax.rem(me - step + n_tp, n_tp)
        else:
            slot = peer_of(me, step, n_tp)
        at = pl.multiple_of(slot * rows, 16)
        project(tokens[pl.ds(at, rows), :], RIM + at)

    @pl.when(seq > 0)
    def _():
        pltpu.make_async_copy(hidden.at[pl.ds(0, RIM)], rim, rim_recv).wait()

    project(rim[...], 0)

    down = lax.broadcasted_iota(jnp.int32, (CHUNK, CHUNK), 0)
    across = lax.broadcasted_iota(jnp.int32, (CHUNK, CHUNK), 1)
    eye = (down == across).astype(jnp.float32)
    wide = lax.broadcasted_iota(jnp.int32, (head_dim, 2 * head_dim), 0) + head_dim
    start = (wide == lax.broadcasted_iota(jnp.int32, (head_dim, 2 * head_dim), 1)).astype(jnp.float32)
    for h in range(heads):
        state[h] = start

    def chunk(c, carry):
        r0 = pl.multiple_of(c * CHUNK, CHUNK)
        scalars = lax.dot_general(
            wdb_ref[...], tokens[pl.ds(r0, CHUNK), :], NT, preferred_element_type=jnp.float32
        )
        per_head = []
        for h in range(heads):
            cols = slice(h * head_dim, (h + 1) * head_dim)
            branch = []
            for b in range(3):
                window = proj[b, pl.ds(r0 + 8, CHUNK + 8), cols]
                conv = jnp.zeros((CHUNK, head_dim), jnp.float32)
                for i in range(taps):
                    offset = 9 - taps + i
                    tap = conv_ref[b, i : i + 1, cols].astype(jnp.float32)
                    conv = conv + window[offset : offset + CHUNK] * tap
                branch.append(silu(conv).astype(jnp.bfloat16).astype(jnp.float32))
            q = unit_rows(branch[0]) * (1.0 / math.sqrt(head_dim))
            k = unit_rows(branch[1])
            v = branch[2]
            u = scalars[h : h + 1, :] + bias_ref[h]
            log_row = -rate_ref[h] * (jnp.maximum(u, 0.0) + jnp.log1p(jnp.exp(-jnp.abs(u))))
            rate_row = 1.0 / (1.0 + jnp.exp(-scalars[heads + h : heads + h + 1, :]))
            cum_col = jnp.sum(jnp.where(across <= down, log_row, 0.0), axis=1, keepdims=True)
            cum_row = jnp.sum(jnp.where(across == down, cum_col, 0.0), axis=0, keepdims=True)
            rate_col = jnp.sum(jnp.where(across == down, rate_row, 0.0), axis=1, keepdims=True)
            end = cum_col[CHUNK - 1 : CHUNK, :]
            gap = jnp.exp(jnp.where(across <= down, cum_col - cum_row, 0.0))
            weight = jnp.where(across <= down, gap, 0.0) * rate_row
            mixing = jnp.where(across < down, weight * dot(k, k, NT), 0.0)
            attend = weight * dot(q, k, NT)
            run = jnp.exp(cum_col)
            tail = rate_col * jnp.exp(end - cum_col)
            per_head.append((q * run, k * run, v, k * tail, mixing, attend, jnp.exp(end)))
        inverse = [eye] * heads
        size = 1
        while size < CHUNK:
            half = (down // size) % 2 == 1
            lower = jnp.logical_and(half, across // size == down // size - 1)
            for h in range(heads):
                part = jnp.where(lower, per_head[h][4], 0.0)
                if size == 1:
                    inverse[h] = eye - part
                else:
                    inverse[h] = inverse[h] - dot(dot(inverse[h], part), inverse[h])
            size *= 2
        for h in range(heads):
            q_run, k_run, v, k_tail, _, attend, fade = per_head[h]
            solved = dot(inverse[h], jnp.concatenate([v, k_run], axis=1))
            held = state[h]
            fresh = solved[:, :head_dim]
            fresh = jnp.concatenate([fresh, jnp.zeros_like(fresh)], axis=1)
            fresh = fresh - dot(solved[:, head_dim:], held)
            read = dot(q_run, held) + dot(attend, fresh)
            state[h] = fade * held + dot(k_tail, fresh, TN)
            outs[h, pl.ds(r0, CHUNK), :] = read[:, :head_dim]
            deltas[h, pl.ds(r0, CHUNK), :] = low(read[:, head_dim:])
        return carry

    lax.fori_loop(0, total // CHUNK, chunk, 0)

    def state_copy(h):
        return pltpu.make_async_remote_copy(
            src_ref=st_out.at[h],
            dst_ref=st_in.at[h],
            send_sem=st_send.at[h],
            recv_sem=st_recv.at[h],
            device_id={"seq": seq + 1},
            device_id_type=MESH,
        )

    for h in range(heads):

        @pl.when(seq > 0)
        def _():
            pltpu.make_async_copy(st_out.at[h], st_in.at[h], st_recv.at[h]).wait()

        @pl.when(seq < last_seq)
        def _():
            mine = state[h]
            st_out[h] = low(mine[:, :head_dim] + dot(mine[:, head_dim:], st_in[h]))
            state_copy(h).start()

    for h in range(heads):
        cols = slice(h * head_dim, (h + 1) * head_dim)
        read = outs[h] + dot(deltas[h], st_in[h])
        scale = lax.rsqrt(jnp.mean(read * read, axis=-1, keepdims=True) + 1e-06)
        gate = silu(proj[3, pl.ds(RIM, total), cols])
        out_ref[:, cols] = low(read * scale * gain_ref[...] * gate)

    for step in range(1, n_tp):
        token_copy(step).wait_send()

    @pl.when(jnp.logical_and(seq < last_seq, me == last_tp))
    def _():
        for target in range(n_tp):
            rim_copy(target).wait_send()

    @pl.when(seq < last_seq)
    def _():
        for h in range(heads):
            state_copy(h).wait_send()


def per_device(
    n_seq, n_tp, hidden, w_qkv, w_gate, w_decay_beta, conv_weight, decay_rate, dt_bias, norm_gain
):
    width = hidden.shape[1]
    heads = decay_rate.shape[0]
    head_dim = norm_gain.shape[0]
    columns = heads * head_dim
    rows = hidden.shape[0]
    total = rows * n_tp
    wdb = w_decay_beta.transpose(1, 2, 0).reshape(2 * heads, width)
    vmem, smem, anywhere = (
        pl.BlockSpec(memory_space=pltpu.VMEM),
        pl.BlockSpec(memory_space=pltpu.SMEM),
        pl.BlockSpec(memory_space=pl.ANY),
    )
    dma = pltpu.SemaphoreType.DMA
    return pl.pallas_call(
        functools.partial(kernel, n_seq, n_tp),
        out_shape=jax.ShapeDtypeStruct((total, columns), jnp.bfloat16),
        in_specs=[smem, smem, anywhere, anywhere, anywhere, vmem, vmem, vmem],
        out_specs=vmem,
        scratch_shapes=[
            pltpu.VMEM((total, width), jnp.bfloat16),
            pltpu.VMEM((RIM, width), jnp.bfloat16),
            pltpu.VMEM((4, width, columns), jnp.bfloat16),
            pltpu.VMEM((4, RIM + total, columns), jnp.float32),
            pltpu.VMEM((heads, head_dim, 2 * head_dim), jnp.float32),
            pltpu.VMEM((heads, total, head_dim), jnp.float32),
            pltpu.VMEM((heads, total, head_dim), jnp.bfloat16),
            pltpu.VMEM((heads, head_dim, head_dim), jnp.bfloat16),
            pltpu.VMEM((heads, head_dim, head_dim), jnp.bfloat16),
            dma((n_tp,)),
            dma((n_tp,)),
            dma((4,)),
            dma((n_tp,)),
            dma,
            dma((heads,)),
            dma((heads,)),
        ],
        compiler_params=pltpu.CompilerParams(
            collective_id=0, has_side_effects=True, vmem_limit_bytes=50 * 1024 * 1024
        ),
    )(
        decay_rate, dt_bias, hidden, w_qkv.transpose(1, 0, 2), w_gate, wdb,
        conv_weight.transpose(1, 0, 2), norm_gain.reshape(1, head_dim),
    )


def solution(mesh):
    return jax.shard_map(
        functools.partial(per_device, mesh.shape["seq"], mesh.shape["tp"]),
        mesh=mesh,
        in_specs=(
            P(("seq", "tp"), None),
            P(None, None, "tp"),
            P(None, "tp"),
            P(None, None, "tp"),
            P(None, None, "tp"),
            P("tp"),
            P("tp"),
            P(),
        ),
        out_specs=P("seq", "tp"),
        check_vma=False,
    )
```

```python
import functools
import math

import jax
import jax.numpy as jnp
from jax import lax
from jax.experimental import pallas as pl
from jax.experimental.pallas import tpu as pltpu
from jax.sharding import PartitionSpec as P

MESH = pl.DeviceIdType.MESH
CHUNK = 128
RIM = 16
NT = (((1,), (1,)), ((), ()))
TN = (((0,), (0,)), ((), ()))


def low(value):
    return value.astype(jnp.bfloat16)


def dot(left, right, dims=(((1,), (0,)), ((), ()))):
    return lax.dot_general(low(left), low(right), dims, preferred_element_type=jnp.float32)


def peer_of(me, step, count):
    if count & (count - 1):
        return lax.rem(me + step, count)
    bit = 1
    while bit < count:
        if step & bit:
            me = me + bit - 2 * bit * lax.rem(me // bit, 2)
        bit *= 2
    return me


def silu(value):
    return value / (1.0 + jnp.exp(-value))


def unit_rows(matrix):
    return matrix * lax.rsqrt(jnp.sum(matrix * matrix, axis=-1, keepdims=True) + 1e-06)


def kernel(
    n_seq, n_tp, rate_hbm, bias_hbm, hidden, w_qkv, w_gate, wdb_hbm, conv_hbm, gain_hbm, out_ref,
    rate_ref, bias_ref, wdb_ref, conv_ref, gain_ref, small_sem,
    tokens, rim, weights, proj, state, outs, deltas, st_in, st_out,
    tok_send, tok_recv, w_sem, rim_send, rim_recv, st_send, st_recv,
    middle, mid_send, mid_recv, solves, q_runs, k_tails, attends, fades,
):
    seq, me = lax.axis_index("seq"), lax.axis_index("tp")
    rows = hidden.shape[0]
    total = tokens.shape[0]
    heads = rate_ref.shape[1]
    head_dim = gain_ref.shape[1]
    taps = conv_ref.shape[1]
    last_tp, last_seq = n_tp - 1, n_seq - 1
    square = n_tp == 4 and rows == CHUNK
    part = rows // 2

    own = pltpu.make_async_copy(hidden, tokens.at[pl.ds(me * rows, rows)], tok_recv.at[0, 0])
    own.start()
    loads = [pltpu.make_async_copy(w_qkv.at[b], weights.at[b], w_sem.at[b]) for b in range(3)]
    loads.append(pltpu.make_async_copy(w_gate, weights.at[3], w_sem.at[3]))
    small = [(rate_hbm, rate_ref), (bias_hbm, bias_ref), (wdb_hbm, wdb_ref), (conv_hbm, conv_ref), (gain_hbm, gain_ref)]
    smalls = [pltpu.make_async_copy(src, dst, small_sem.at[i]) for i, (src, dst) in enumerate(small)]
    for load in loads + smalls:
        load.start()

    barrier = pltpu.get_barrier_semaphore()

    def greet(where):
        pl.semaphore_signal(barrier, inc=1, device_id=where, device_id_type=MESH)

    for step in range(1, n_tp):
        greet({"tp": peer_of(me, step, n_tp)})

    @pl.when(seq > 0)
    def _():
        greet({"seq": seq - 1})

        @pl.when(me < last_tp)
        def _():
            greet({"seq": seq - 1, "tp": last_tp})

    @pl.when(seq < last_seq)
    def _():
        greet({"seq": seq + 1})

    before = (seq + last_seq) // n_seq
    after = (2 * last_seq - seq) // n_seq
    tail_owner = (me + 1) // n_tp
    pl.semaphore_wait(barrier, last_tp + before + after + after * tail_owner * last_tp)

    def token_copy(step):
        return pltpu.make_async_remote_copy(
            src_ref=hidden,
            dst_ref=tokens.at[pl.ds(me * rows, rows)],
            send_sem=tok_send.at[step, 0],
            recv_sem=tok_recv.at[step, 0],
            device_id={"tp": peer_of(me, step, n_tp)},
            device_id_type=MESH,
        )

    def part_copy(step, half):
        return pltpu.make_async_remote_copy(
            src_ref=hidden.at[pl.ds(half * part, part)],
            dst_ref=tokens.at[pl.ds(me * rows + half * part, part)],
            send_sem=tok_send.at[step, half],
            recv_sem=tok_recv.at[step, half],
            device_id={"tp": peer_of(me, step, n_tp)},
            device_id_type=MESH,
        )

    def relay_copy(half):
        there = tokens.at[pl.ds(peer_of(me, 2 - half, n_tp) * rows + half * part, part)]
        return pltpu.make_async_remote_copy(
            src_ref=there,
            dst_ref=there,
            send_sem=tok_send.at[3, half],
            recv_sem=tok_recv.at[3, half],
            device_id={"tp": peer_of(me, 1 + half, n_tp)},
            device_id_type=MESH,
        )

    def middle_copy(target):
        return pltpu.make_async_remote_copy(
            src_ref=hidden.at[pl.ds(rows - RIM, RIM)],
            dst_ref=middle,
            send_sem=mid_send.at[target - 2],
            recv_sem=mid_recv,
            device_id={"tp": target},
            device_id_type=MESH,
        )

    def rim_copy(target):
        return pltpu.make_async_remote_copy(
            src_ref=hidden.at[pl.ds(rows - RIM, RIM)],
            dst_ref=rim,
            send_sem=rim_send.at[target],
            recv_sem=rim_recv,
            device_id={"seq": seq + 1, "tp": target},
            device_id_type=MESH,
        )

    @pl.when(jnp.logical_and(seq < last_seq, me == last_tp))
    def _():
        for target in range(n_tp):
            rim_copy(target).start()

    if square:

        @pl.when(me == 1)
        def _():
            for target in (2, 3):
                middle_copy(target).start()

        for step, half in ((1, 1), (2, 0), (1, 0), (2, 1)):
            part_copy(step, half).start()
    else:
        for step in range(1, n_tp):
            token_copy(step).start()

    @pl.when(seq == 0)
    def _():
        rim[...] = jnp.zeros_like(rim)
        st_in[...] = jnp.zeros_like(st_in)

    for load in loads + smalls:
        load.wait()

    def project(block, at):
        def one(b, carry):
            full = jnp.dot(block, weights[b], preferred_element_type=jnp.float32)
            rounded = full.astype(jnp.bfloat16).astype(jnp.float32)
            proj[b, pl.ds(pl.multiple_of(at, 16), block.shape[0]), :] = jnp.where(b < 3, rounded, full)
            return carry

        lax.fori_loop(0, 4, one, 0)

    def project_slot(slot):
        at = pl.multiple_of(slot * rows, 16)
        project(tokens[pl.ds(at, rows), :], RIM + at)

    def project_rim():
        @pl.when(seq > 0)
        def _():
            pltpu.make_async_copy(hidden.at[pl.ds(0, RIM)], rim, rim_recv).wait()

        project(rim[...], 0)

    down = lax.broadcasted_iota(jnp.int32, (CHUNK, CHUNK), 0)
    across = lax.broadcasted_iota(jnp.int32, (CHUNK, CHUNK), 1)
    eye = (down == across).astype(jnp.float32)
    wide = lax.broadcasted_iota(jnp.int32, (head_dim, 2 * head_dim), 0) + head_dim
    start = (wide == lax.broadcasted_iota(jnp.int32, (head_dim, 2 * head_dim), 1)).astype(jnp.float32)
    for h in range(heads):
        state[h] = start

    wdb = low(jnp.concatenate([wdb_ref[0].astype(jnp.float32), wdb_ref[1].astype(jnp.float32)], axis=0))

    def prepare(c):
        r0 = pl.multiple_of(c * CHUNK, CHUNK)
        scalars = lax.dot_general(
            wdb, tokens[pl.ds(r0, CHUNK), :], NT, preferred_element_type=jnp.float32
        )
        per_head = []
        for h in range(heads):
            cols = slice(h * head_dim, (h + 1) * head_dim)
            branch = []
            for b in range(3):
                window = proj[b, pl.ds(r0 + 8, CHUNK + 8), cols]
                conv = jnp.zeros((CHUNK, head_dim), jnp.float32)
                for i in range(taps):
                    offset = 9 - taps + i
                    tap = conv_ref[b, i : i + 1, cols].astype(jnp.float32)
                    conv = conv + window[offset : offset + CHUNK] * tap
                branch.append(silu(conv).astype(jnp.bfloat16).astype(jnp.float32))
            q = unit_rows(branch[0]) * (1.0 / math.sqrt(head_dim))
            k = unit_rows(branch[1])
            v = branch[2]
            u = scalars[h : h + 1, :] + bias_ref[0:1, h : h + 1]
            log_row = -rate_ref[0:1, h : h + 1] * (jnp.maximum(u, 0.0) + jnp.log1p(jnp.exp(-jnp.abs(u))))
            rate_row = 1.0 / (1.0 + jnp.exp(-scalars[heads + h : heads + h + 1, :]))
            cum_col = jnp.sum(jnp.where(across <= down, log_row, 0.0), axis=1, keepdims=True)
            cum_row = jnp.sum(jnp.where(across == down, cum_col, 0.0), axis=0, keepdims=True)
            rate_col = jnp.sum(jnp.where(across == down, rate_row, 0.0), axis=1, keepdims=True)
            end = cum_col[CHUNK - 1 : CHUNK, :]
            gap = jnp.exp(jnp.where(across <= down, cum_col - cum_row, 0.0))
            weight = jnp.where(across <= down, gap, 0.0) * rate_row
            mixing = jnp.where(across < down, weight * dot(k, k, NT), 0.0)
            attend = weight * dot(q, k, NT)
            run = jnp.exp(cum_col)
            tail = rate_col * jnp.exp(end - cum_col)
            q_runs[c, h] = low(q * run)
            k_tails[c, h] = low(k * tail)
            attends[c, h] = low(attend)
            fades[c, h] = jnp.broadcast_to(jnp.exp(end), (1, head_dim))
            per_head.append((mixing, low(jnp.concatenate([v, k * run], axis=1))))
        return per_head

    def local(chunks):
        chains = [(c, h) + item for c in chunks for h, item in enumerate(prepare(c))]
        inverse = [None] * len(chains)
        size = 1
        while size < CHUNK:
            half = (down // size) % 2 == 1
            lower = jnp.logical_and(half, across // size == down // size - 1)
            for i, (_, _, mixing, _) in enumerate(chains):
                corner = jnp.where(lower, mixing, 0.0)
                if size == 1:
                    inverse[i] = eye - corner
                else:
                    inverse[i] = inverse[i] - dot(dot(inverse[i], corner), inverse[i])
            size *= 2
        for i, (c, h, _, right) in enumerate(chains):
            solves[c, h] = dot(inverse[i], right)

    def advance(c, carry):
        r0 = pl.multiple_of(c * CHUNK, CHUNK)
        for h in range(heads):
            solved = solves[c, h]
            held = state[h]
            fresh = solved[:, :head_dim]
            fresh = jnp.concatenate([fresh, jnp.zeros_like(fresh)], axis=1)
            fresh = fresh - dot(solved[:, head_dim:], held)
            read = dot(q_runs[c, h], held) + dot(attends[c, h], fresh)
            fade = jnp.concatenate([fades[c, h]] * 2, axis=1)
            state[h] = fade * held + dot(k_tails[c, h], fresh, TN)
            outs[h, pl.ds(r0, CHUNK), :] = read[:, :head_dim]
            deltas[h, pl.ds(r0, CHUNK), :] = low(read[:, head_dim:])
        return carry

    count = total // CHUNK
    own.wait()
    project_slot(me)
    if square:
        part_copy(1, 1).wait_recv()
        relay_copy(1).start()
        part_copy(2, 0).wait_recv()
        relay_copy(0).start()
        project_rim()

        @pl.when(me >= 2)
        def _():
            pltpu.make_async_copy(hidden.at[pl.ds(0, RIM)], middle, mid_recv).wait()
            project(middle[...], 2 * rows)

        part_copy(1, 0).wait_recv()
        project_slot(peer_of(me, 1, n_tp))
        first = 2 * (me // 2)
        local((first, first + 1))
        part_copy(2, 1).wait_recv()
        project_slot(peer_of(me, 2, n_tp))
        relay_copy(0).wait_recv()
        relay_copy(1).wait_recv()
        project_slot(peer_of(me, 3, n_tp))
        local((2 - first, 3 - first))
    else:
        for step in range(1, n_tp):
            token_copy(step).wait_recv()
            if n_tp & (n_tp - 1):
                project_slot(lax.rem(me - step + n_tp, n_tp))
            else:
                project_slot(peer_of(me, step, n_tp))
        project_rim()
        lax.fori_loop(0, count, lambda c, carry: (local((c,)), carry)[1], 0)
    lax.fori_loop(0, count, advance, 0)

    def state_copy(h):
        return pltpu.make_async_remote_copy(
            src_ref=st_out.at[h],
            dst_ref=st_in.at[h],
            send_sem=st_send.at[h],
            recv_sem=st_recv.at[h],
            device_id={"seq": seq + 1},
            device_id_type=MESH,
        )

    for h in range(heads):

        @pl.when(seq > 0)
        def _():
            pltpu.make_async_copy(st_out.at[h], st_in.at[h], st_recv.at[h]).wait()

        @pl.when(seq < last_seq)
        def _():
            mine = state[h]
            st_out[h] = low(mine[:, :head_dim] + dot(mine[:, head_dim:], st_in[h]))
            state_copy(h).start()

    for h in range(heads):
        cols = slice(h * head_dim, (h + 1) * head_dim)
        read = outs[h] + dot(deltas[h], st_in[h])
        scale = lax.rsqrt(jnp.mean(read * read, axis=-1, keepdims=True) + 1e-06)
        gate = silu(proj[3, pl.ds(RIM, total), cols])
        out_ref[:, cols] = low(read * scale * gain_ref[...] * gate)

    if square:
        for half in range(2):
            part_copy(1, half).wait_send()
            part_copy(2, half).wait_send()
            relay_copy(half).wait_send()

        @pl.when(me == 1)
        def _():
            for target in (2, 3):
                middle_copy(target).wait_send()
    else:
        for step in range(1, n_tp):
            token_copy(step).wait_send()

    @pl.when(jnp.logical_and(seq < last_seq, me == last_tp))
    def _():
        for target in range(n_tp):
            rim_copy(target).wait_send()

    @pl.when(seq < last_seq)
    def _():
        for h in range(heads):
            state_copy(h).wait_send()


def per_device(
    n_seq, n_tp, hidden, w_qkv, w_gate, w_decay_beta, conv_weight, decay_rate, dt_bias, norm_gain
):
    width = hidden.shape[1]
    heads = decay_rate.shape[0]
    head_dim = norm_gain.shape[0]
    columns = heads * head_dim
    rows = hidden.shape[0]
    total = rows * n_tp
    vmem, anywhere = pl.BlockSpec(memory_space=pltpu.VMEM), pl.BlockSpec(memory_space=pl.ANY)
    dma = pltpu.SemaphoreType.DMA
    count = total // CHUNK
    return pl.pallas_call(
        functools.partial(kernel, n_seq, n_tp),
        out_shape=jax.ShapeDtypeStruct((total, columns), jnp.bfloat16),
        in_specs=[anywhere] * 8,
        out_specs=vmem,
        scratch_shapes=[
            pltpu.VMEM((1, heads), jnp.float32),
            pltpu.VMEM((1, heads), jnp.float32),
            pltpu.VMEM((2, heads, width), jnp.bfloat16),
            pltpu.VMEM((3, conv_weight.shape[0], columns), jnp.bfloat16),
            pltpu.VMEM((1, head_dim), jnp.float32),
            dma((5,)),
            pltpu.VMEM((total, width), jnp.bfloat16),
            pltpu.VMEM((RIM, width), jnp.bfloat16),
            pltpu.VMEM((4, width, columns), jnp.bfloat16),
            pltpu.VMEM((4, RIM + total, columns), jnp.float32),
            pltpu.VMEM((heads, head_dim, 2 * head_dim), jnp.float32),
            pltpu.VMEM((heads, total, head_dim), jnp.float32),
            pltpu.VMEM((heads, total, head_dim), jnp.bfloat16),
            pltpu.VMEM((heads, head_dim, head_dim), jnp.bfloat16),
            pltpu.VMEM((heads, head_dim, head_dim), jnp.bfloat16),
            dma((n_tp, 2)),
            dma((n_tp, 2)),
            dma((4,)),
            dma((n_tp,)),
            dma,
            dma((heads,)),
            dma((heads,)),
            pltpu.VMEM((RIM, width), jnp.bfloat16),
            dma((2,)),
            dma,
            pltpu.VMEM((count, heads, CHUNK, 2 * head_dim), jnp.float32),
            pltpu.VMEM((count, heads, CHUNK, head_dim), jnp.bfloat16),
            pltpu.VMEM((count, heads, CHUNK, head_dim), jnp.bfloat16),
            pltpu.VMEM((count, heads, CHUNK, CHUNK), jnp.bfloat16),
            pltpu.VMEM((count, heads, 1, head_dim), jnp.float32),
        ],
        compiler_params=pltpu.CompilerParams(
            collective_id=0, has_side_effects=True, vmem_limit_bytes=60 * 1024 * 1024
        ),
    )(
        decay_rate.reshape(1, heads), dt_bias.reshape(1, heads), hidden,
        w_qkv.transpose(1, 0, 2), w_gate, w_decay_beta.transpose(1, 2, 0),
        conv_weight.transpose(1, 0, 2), norm_gain.reshape(1, head_dim),
    )


def solution(mesh):
    return jax.shard_map(
        functools.partial(per_device, mesh.shape["seq"], mesh.shape["tp"]),
        mesh=mesh,
        in_specs=(
            P(("seq", "tp"), None),
            P(None, None, "tp"),
            P(None, "tp"),
            P(None, None, "tp"),
            P(None, None, "tp"),
            P("tp"),
            P("tp"),
            P(),
        ),
        out_specs=P("seq", "tp"),
        check_vma=False,
    )
```
